32 devices in a mesh: dp: 4 (over y, x), expert: 8 (over z, core).
Axes of the slice: x: 2, y: 2, z: 4, core: 2. Of those that a mesh axis runs over, the one named last changes fastest.
Arguments:
- tokens: bfloat16 [4096, 4096], P(('dp', 'expert')), may hold values from -6 to 6
- routes: int32 [4096, 2], P(('dp', 'expert')), may hold values from 0 to 7, all different within a row; in each aligned block of 128 rows (0 to 127, 128 to 255, ...) at most 48 rows name the same one
- router_weight: bfloat16 [4096, 8], replicated, may hold values from -0.09375 to 0.09375
- shift: float32 [1, 4096], replicated, may hold values from -3 to 3
- scale: float32 [1, 4096], replicated, may hold values from -3 to 3
- gate_mod: float32 [1, 4096], replicated, may hold values from -4 to 4
- gate_weight: bfloat16 [8, 4096, 1024], P(None, ('dp', 'expert')), may hold values from -0.09375 to 0.09375
- up_weight: bfloat16 [8, 4096, 1024], P(None, ('dp', 'expert')), may hold values from -0.09375 to 0.09375
- down_weight: bfloat16 [8, 4096, 1024], P(None, ('dp', 'expert')), may hold values from -0.1875 to 0.1875
Outputs:
- update: bfloat16 [4096, 4096], P(('dp', 'expert'))
The draws below stay inside these ranges and needn't reach their ends.
Inputs may be any that keep to these rules, and one draw needn't show every extreme that they name: `routes`: each row names two different experts; among the rows of one device no expert is named more than 48 times, a bound that some block reaches.
All inputs are finite; a program needn't handle non-finite values.
Results may differ from the reference program's by a relative error of at most 0.0072.
Values may be sent and summed in bfloat16 or wider, within the bound.
A program may use at most 128 MiB of HBM per device.

```python
import math
import jax
import jax.numpy as jnp
import numpy as np
from jax import lax

D = 4096
FE = 1024
E = 8
TOK_DEV = 128
CAP = 48
PIX = 4096
TOKENS = 4096
IMAGES = 1


def steps_of(key, extent, cuts, least, high):
    level, own = 1.0, jax.random.fold_in(key, 6)
    for dim, blocks in cuts:
        steps = jnp.exp(jax.random.uniform(jax.random.fold_in(own, dim), (blocks,), jnp.float32, least / len(cuts), high / len(cuts)))
        level = level * jnp.repeat(steps, extent[dim] // blocks).reshape([-1 if axis == dim else 1 for axis in range(len(extent))])
    return level


def routed_block(rng, own, number, rows, count, top, limit, skew):
    order = jax.random.permutation(rng, count)
    crowded, usual = shares(count, rows * top, limit, skew, True), shares(count, rows * top, limit, skew, False)
    places = jnp.arange(count)

    def named(tallies, turn):
        used = int((tallies > 0).sum())
        fixed = max(1, used // 4)
        moved = fixed + (places - fixed + turn * (used - fixed)) % max(1, count - fixed)
        return jnp.zeros((count,), jnp.int32).at[order[jnp.where(places < fixed, places, moved)]].set(jnp.asarray(tallies, jnp.int32))

    tallies = jnp.where(number % 4 == 0, named(crowded, number // 4), named(usual, number - number // 4 - 1))
    mixed = jax.random.permutation(jax.random.fold_in(own, 3), count)
    donor, receiver = mixed[0:count // 2 * 2:2], mixed[1:count // 2 * 2:2]
    margin = jnp.minimum(tallies[donor] - 1, limit - tallies[receiver]) // 2
    margin = jnp.where((donor == order[0]) | (receiver == order[0]) | (tallies[receiver] == 0), 0, jnp.maximum(margin, 0))
    moved = jax.random.randint(jax.random.fold_in(own, 4), (count // 2,), 0, 1 << 20) % (margin + 1)
    tallies = tallies.at[donor].add(-moved).at[receiver].add(moved)
    labels = jnp.searchsorted(jnp.cumsum(tallies), jnp.arange(rows * top), side="right").astype(jnp.int32)
    listing = labels.reshape(top, rows).T
    listing = listing[jax.random.permutation(jax.random.fold_in(own, 1), rows)]
    turn = jax.random.randint(jax.random.fold_in(own, 2), (rows, 1), 0, top)
    return jnp.take_along_axis(listing, (jnp.arange(top)[None, :] + turn) % top, axis=1)


def shares(number_of, total, reach, lean, full):
    loads = [(1 << 20) // math.isqrt(rank ** lean) + 1 for rank in range(1, number_of + 1)]
    largest = reach if full else min(reach, max(-(-total // number_of), total * loads[0] // sum(loads)))
    least = 1 if total - largest >= number_of - 1 else 0
    given, rest = [largest] + [least] * (number_of - 1), total - largest - least * (number_of - 1)
    while rest > 0:
        candidates = [i for i in range(1, number_of) if given[i] < largest] or [i for i in range(1, number_of) if given[i] < reach]
        mass, budget = sum([loads[i] for i in candidates]), rest
        for i in candidates:
            addition = min(reach - given[i], max(1, budget * loads[i] // mass), rest)
            given[i] = given[i] + addition
            rest = rest - addition
    return np.array(given)


def gaussian(rng, shape, scale, bound, pieces=(), kind=jnp.bfloat16):
    factor_of = steps_of(rng, shape, pieces, -0.22, 0.18) if pieces else 1.0
    result = jax.random.normal(rng, shape, jnp.float32) * scale * factor_of
    return jnp.minimum(jnp.maximum(result, -bound), bound).astype(kind)


def setup_inputs(seed: int = 0) -> dict:
    arg_keys = jax.random.split(jax.random.key(seed), 10)
    tokens = gaussian(arg_keys[0], (TOKENS, D), 1.0, 6.0, ((0, 32),))
    routes_keys = jax.random.split(jax.random.fold_in(arg_keys[1], 1), TOKENS // TOK_DEV)
    routes_turns = jax.random.permutation(jax.random.fold_in(arg_keys[1], 3), TOKENS // TOK_DEV)
    routes = jax.vmap(lambda own, number: routed_block(jax.random.fold_in(arg_keys[1], 2), own, number, TOK_DEV, E, 2, CAP, 2))(routes_keys, routes_turns).reshape((TOKENS, 2))
    router_weight = gaussian(arg_keys[2], (D, E), D ** -0.5, 0.09375)
    shift = gaussian(arg_keys[3], (IMAGES, D), 0.5, 3.0, (), jnp.float32)
    scale = gaussian(arg_keys[4], (IMAGES, D), 0.5, 3.0, (), jnp.float32)
    gate_mod = gaussian(arg_keys[5], (IMAGES, D), 1.0, 4.0, (), jnp.float32)
    gate_weight = gaussian(arg_keys[6], (E, D, FE), D ** -0.5, 0.09375, ((1, 32),))
    up_weight = gaussian(arg_keys[7], (E, D, FE), D ** -0.5, 0.09375, ((1, 32),))
    down_weight = gaussian(arg_keys[8], (E, D, FE), FE ** -0.5, 0.1875, ((1, 32),))
    return dict(tokens=tokens, routes=routes, router_weight=router_weight, shift=shift, scale=scale, gate_mod=gate_mod, gate_weight=gate_weight, up_weight=up_weight, down_weight=down_weight)


EPS = 1e-06

def reference(tokens, routes, router_weight, shift, scale, gate_mod, gate_weight, up_weight, down_weight):
    blocks = TOKENS // TOK_DEV

    def norm_image(items):
        rows, image_shift, image_scale = items
        values = rows.astype(jnp.float32)
        meansq = lax.optimization_barrier(jnp.mean(values * values, axis=-1, keepdims=True))
        normed_rows = values * lax.rsqrt(meansq + EPS) * (1.0 + image_scale[None, :]) + image_shift[None, :]
        normed_rows = normed_rows.astype(jnp.bfloat16)
        logit_rows = jnp.dot(normed_rows, router_weight, preferred_element_type=jnp.float32)
        return (normed_rows, logit_rows)
    normed, logits = lax.map(norm_image, (tokens.reshape(IMAGES, PIX, D), shift, scale))
    normed = normed.reshape(TOKENS, D)
    logits = logits.reshape(TOKENS, E)
    chosen = jnp.take_along_axis(logits, routes, axis=1)
    score_flat = jax.nn.sigmoid(chosen).reshape(-1)
    flat = routes.reshape(blocks, 2 * TOK_DEV)
    hot = (flat[:, :, None] == jnp.arange(E, dtype=jnp.int32)[None, None, :]).astype(jnp.int32)
    rank = (jnp.cumsum(hot, axis=1) - hot).astype(jnp.int32)
    slot = lax.optimization_barrier(jnp.sum(rank * hot, axis=-1)).astype(jnp.int32)
    position = (flat * CAP + slot).astype(jnp.int32)
    global_ids = (jnp.arange(blocks, dtype=jnp.int32)[:, None] * (2 * TOK_DEV) + jnp.arange(2 * TOK_DEV, dtype=jnp.int32)[None, :]).astype(jnp.int32)

    def fill_table(where_to, ids):
        return jnp.full((E * CAP,), -1, jnp.int32).at[where_to].set(ids)
    table = jax.vmap(fill_table)(position, global_ids)
    table = table.reshape(blocks, E, CAP).transpose(1, 0, 2).reshape(E, blocks * CAP)

    def expert_step(total, items):
        ids, w_gate, w_up, w_down = items
        filled = ids >= 0
        safe = jnp.where(filled, ids, 0).astype(jnp.int32)
        token_ids = (safe // 2).astype(jnp.int32)
        rows = jnp.where(filled[:, None], normed[token_ids], jnp.zeros((), jnp.bfloat16))
        gate = jnp.dot(rows, w_gate, preferred_element_type=jnp.float32)
        upper = jnp.dot(rows, w_up, preferred_element_type=jnp.float32)
        hidden = (jax.nn.silu(gate) * upper).astype(jnp.bfloat16)
        output = jnp.dot(hidden, w_down.T, preferred_element_type=jnp.float32).astype(jnp.bfloat16)
        weight = jnp.where(filled, score_flat[safe], jnp.zeros((), jnp.float32))
        total = total.at[token_ids].add(weight[:, None] * output.astype(jnp.float32))
        return (total, None)
    total, unused = lax.scan(expert_step, jnp.zeros((TOKENS, D), jnp.float32), (table, gate_weight, up_weight, down_weight))
    update = total.reshape(IMAGES, PIX, D) * gate_mod[:, None, :]
    return update.reshape(TOKENS, D).astype(jnp.bfloat16)
```

```python
import functools

import jax
import jax.numpy as jnp
from jax import lax
from jax.experimental import pallas as pl
from jax.experimental.pallas import tpu as pltpu
from jax.sharding import PartitionSpec as P

PIX = 4096


EPS = 1e-06


def send_back(output):
    return lax.all_to_all(output, "expert", split_axis=0, concat_axis=0, tiled=True)


def shards_plain(
    tokens, routes, router_weight, shift, scale, gate_mod, gate_weight, up_weight, down_weight
):
    tok_dev = tokens.shape[0]
    width = tokens.shape[1]
    experts = router_weight.shape[1]
    n_owner = lax.axis_size("expert")
    local_count = experts // n_owner
    capacity = max(2, 3 * tok_dev // experts)
    first_row = (lax.axis_index("dp") * n_owner + lax.axis_index("expert")) * tok_dev
    image = first_row // PIX
    shift_row = lax.dynamic_slice_in_dim(shift, image, 1, 0)
    scale_row = lax.dynamic_slice_in_dim(scale, image, 1, 0)
    gate_row = lax.dynamic_slice_in_dim(gate_mod, image, 1, 0)
    values = tokens.astype(jnp.float32)
    meansq = jnp.mean(values * values, axis=-1, keepdims=True)
    normed = (values * lax.rsqrt(meansq + EPS) * (1.0 + scale_row) + shift_row).astype(jnp.bfloat16)
    logits = jnp.dot(normed, router_weight, preferred_element_type=jnp.float32)
    onehot = routes[:, :, None] == jnp.arange(experts, dtype=jnp.int32)[None, None, :]
    chosen = jnp.sum(jnp.where(onehot, logits[:, None, :], 0.0), axis=-1)
    score = jax.nn.sigmoid(chosen)
    flat = routes.reshape(-1)
    hot = (flat[:, None] == jnp.arange(experts, dtype=jnp.int32)[None, :]).astype(jnp.int32)
    rank = jnp.cumsum(hot, axis=0) - hot
    slot = jnp.sum(rank * hot, axis=-1)
    position = flat * capacity + slot
    source = (
        jnp.zeros((experts * capacity,), jnp.int32)
        .at[position]
        .set(jnp.arange(2 * tok_dev, dtype=jnp.int32) // 2)
    )
    filled = jnp.zeros((experts * capacity,), jnp.bool_).at[position].set(True)
    outgoing = jnp.where(filled[:, None], normed[source], jnp.zeros((), jnp.bfloat16)).reshape(
        experts, capacity, width
    )
    quarter_gate, quarter_up, quarter_down = (
        lax.all_to_all(gate_weight, "expert", split_axis=0, concat_axis=1, tiled=True),
        lax.all_to_all(up_weight, "expert", split_axis=0, concat_axis=1, tiled=True),
        lax.all_to_all(down_weight, "expert", split_axis=0, concat_axis=1, tiled=True),
    )
    w_gate, w_up, w_down = (
        lax.all_gather(quarter_gate, "dp", axis=1, tiled=True),
        lax.all_gather(quarter_up, "dp", axis=1, tiled=True),
        lax.all_gather(quarter_down, "dp", axis=1, tiled=True),
    )
    received = lax.all_to_all(outgoing, "expert", split_axis=0, concat_axis=0, tiled=True)
    slots = received.shape[1]
    grid = received.reshape(n_owner, local_count, slots, width)
    gate = jnp.einsum("nxcd,xdf->nxcf", grid, w_gate, preferred_element_type=jnp.float32)
    upper = jnp.einsum("nxcd,xdf->nxcf", grid, w_up, preferred_element_type=jnp.float32)
    hidden = (jax.nn.silu(gate) * upper).astype(jnp.bfloat16)
    output = jnp.einsum(
        "nxcf,xdf->nxcd", hidden, w_down, preferred_element_type=jnp.float32
    ).astype(jnp.bfloat16)
    output = output.reshape(n_owner * local_count, slots, width)
    incoming = send_back(output)
    picked = (
        incoming.reshape(experts * capacity, width)[position]
        .astype(jnp.float32)
        .reshape(tok_dev, 2, width)
    )
    branch = jnp.sum(score[:, :, None] * picked, axis=1)
    return (gate_row * branch).astype(jnp.bfloat16)


MESH = pl.DeviceIdType.MESH


def wait_bytes(ref, sem):
    pltpu.make_async_copy(ref, ref, sem).wait()


def kernel(
    n_dp, n_owner, tok_ref, router_ref, routes_ref, shift_ref, scale_ref, gmod_ref, disp_ref, comb_ref,
    gate_ref, up_ref, down_ref, out_ref,
    weights, normed, outgoing, rows, gate_acc, hidden, obuf, incoming, score_ref,
    z_send, w_recv, xy_send, t_send, t_recv, o_send, o_recv,
):
    dp, me = lax.axis_index("dp"), lax.axis_index("expert")
    x_dp = dp + 1 - 2 * (dp % 2)
    y_dp = (dp + 2) % n_dp
    d_dp = n_dp - 1 - dp
    tok_dev, width = tok_ref.shape
    capacity = disp_ref.shape[1]
    depth, units = gate_ref.shape[1], gate_ref.shape[2]
    args = (gate_ref, up_ref, down_ref)

    barrier = pltpu.get_barrier_semaphore()
    for r in range(1, n_owner):
        pl.semaphore_signal(barrier, inc=1, device_id=(dp, (me + r) % n_owner), device_id_type=MESH)
    pl.semaphore_signal(barrier, inc=1, device_id=(x_dp, me), device_id_type=MESH)
    pl.semaphore_signal(barrier, inc=1, device_id=(y_dp, me), device_id_type=MESH)
    pl.semaphore_wait(barrier, n_owner + 1)

    def own(a):
        return pltpu.make_async_copy(args[a].at[me], weights.at[a, dp * n_owner + me], w_recv.at[a, 0, 0])

    def send_column(a):
        own(a).start()
        for r in range(1, n_owner):
            to = (me + r) % n_owner
            pltpu.make_async_remote_copy(
                src_ref=args[a].at[to], dst_ref=weights.at[a, dp * n_owner + me],
                send_sem=z_send.at[a], recv_sem=w_recv.at[a, r, 0],
                device_id=(dp, to), device_id_type=MESH,
            ).start()

    def piece(a, r, part):
        return weights.at[a, part * n_owner + (me + n_owner - r) % n_owner]

    def spread(a, r, part, to, slot, kind):
        pltpu.make_async_remote_copy(
            src_ref=piece(a, r, part), dst_ref=piece(a, r, part),
            send_sem=xy_send.at[a, kind], recv_sem=w_recv.at[a, r, slot],
            device_id=(to, me), device_id_type=MESH,
        ).start()

    def arrived(a, r, part, slot):
        wait_bytes(piece(a, r, part), w_recv.at[a, r, slot])

    def relay(a, r):
        arrived(a, r, dp, 0)
        spread(a, r, dp, x_dp, 1, 0)
        spread(a, r, dp, y_dp, 2, 1)

    def corner(a, r):
        arrived(a, r, x_dp, 1)
        if r % 2 == 0:
            spread(a, r, x_dp, y_dp, 3, 2)
        arrived(a, r, y_dp, 2)
        if r % 2 == 1:
            spread(a, r, y_dp, x_dp, 3, 2)

    send_column(0)
    relay(0, 0)

    block = 16

    @pl.loop(0, tok_dev // block)
    def _(i):
        at = pl.ds(pl.multiple_of(i * block, block), block)
        values = tok_ref[at, :].astype(jnp.float32)
        meansq = jnp.mean(values * values, axis=-1, keepdims=True)
        fresh = values * lax.rsqrt(meansq + EPS) * (1.0 + scale_ref[...]) + shift_ref[...]
        normed[at, :] = fresh.astype(jnp.bfloat16)

    for r in range(n_owner):
        to = (me + r) % n_owner
        picked = jnp.dot(disp_ref[to], normed[...], preferred_element_type=jnp.float32).astype(jnp.bfloat16)
        if r == 0:
            rows[me] = picked
        else:
            outgoing[r - 1] = picked
            pltpu.make_async_remote_copy(
                src_ref=outgoing.at[r - 1], dst_ref=rows.at[me],
                send_sem=t_send.at[0], recv_sem=t_recv.at[r],
                device_id=(dp, to), device_id_type=MESH,
            ).start()
    send_column(1)
    send_column(2)

    logits = jnp.dot(normed[...], router_ref[...], preferred_element_type=jnp.float32)
    names = lax.broadcasted_iota(jnp.int32, logits.shape, 1)
    for k in range(2):
        chosen = jnp.sum(jnp.where(routes_ref[:, k : k + 1] == names, logits, 0.0), axis=-1, keepdims=True)
        score_ref[k] = jnp.broadcast_to(jax.nn.sigmoid(chosen), score_ref.shape[1:])

    tile = 256

    def product(a, at):
        part = weights[a, :, :, at].reshape(width, tile)
        grid = rows[...].reshape(n_owner * capacity, width)
        return jnp.dot(grid, part, preferred_element_type=jnp.float32)

    lag = 2
    for a in range(2):
        for r in range(n_owner + lag):
            if 0 < r < n_owner:
                relay(a, r)
            if r >= lag:
                corner(a, r - lag)
        for r in range(n_owner):
            arrived(a, r, d_dp, 3)
        relay(a + 1, 0)
        if a == 0:
            for r in range(1, n_owner):
                wait_bytes(rows.at[(me + n_owner - r) % n_owner], t_recv.at[r])

        @pl.loop(0, units // tile)
        def _(i):
            at = pl.ds(pl.multiple_of(i * tile, tile), tile)
            if a == 0:
                gate_acc[:, at] = product(0, at)
            else:
                gate = gate_acc[:, at]
                hidden[:, at] = (jax.nn.silu(gate) * product(1, at)).astype(jnp.bfloat16)

    def finish(r):
        arrived(2, r, d_dp, 3)
        source = (me + n_owner - r) % n_owner
        for q in range(n_dp):
            part = weights[2, q * n_owner + source]
            result = lax.dot_general(
                hidden[...], part, (((1,), (1,)), ((), ())), preferred_element_type=jnp.float32
            ).astype(jnp.bfloat16)
            obuf[r, :, :, q * depth : (q + 1) * depth] = result.reshape(n_owner, capacity, depth)
        incoming[source, me] = obuf[r, me]
        for t in range(1, n_owner):
            to = (me + t) % n_owner
            pltpu.make_async_remote_copy(
                src_ref=obuf.at[r, to], dst_ref=incoming.at[source, me],
                send_sem=o_send.at[r], recv_sem=o_recv.at[r, t],
                device_id=(dp, to), device_id_type=MESH,
            ).start()

    far = 2
    for r in range(n_owner + lag + far):
        if 0 < r < n_owner:
            relay(2, r)
        if lag <= r < n_owner + lag:
            corner(2, r - lag)
        if r >= lag + far:
            finish(r - lag - far)

    for r in range(n_owner):
        for t in range(1, n_owner):
            sender = (me + n_owner - t) % n_owner
            source = (me + 2 * n_owner - t - r) % n_owner
            wait_bytes(incoming.at[source, sender], o_recv.at[r, t])

    for source in range(n_owner):
        block_in = incoming[source].reshape(n_owner * capacity, n_dp * depth)
        first = jnp.dot(comb_ref[0], block_in, preferred_element_type=jnp.float32)
        second = jnp.dot(comb_ref[1], block_in, preferred_element_type=jnp.float32)
        for q in range(n_dp):
            cols = slice(q * depth, (q + 1) * depth)
            at = slice((q * n_owner + source) * depth, (q * n_owner + source + 1) * depth)
            branch = score_ref[0] * first[:, cols] + score_ref[1] * second[:, cols]
            out_ref[:, at] = (gmod_ref[:, at] * branch).astype(jnp.bfloat16)

    for a in range(3):
        wait_bytes(args[a].at[pl.ds(0, n_owner - 1)], z_send.at[a])
        for kind in range(3):
            wait_bytes(weights.at[a, pl.ds(0, n_owner)], xy_send.at[a, kind])
    wait_bytes(outgoing, t_send.at[0])
    for r in range(n_owner):
        wait_bytes(obuf.at[r, pl.ds(0, n_owner - 1)], o_send.at[r])


def shards(
    n_dp, n_owner, tokens, routes, router_weight, shift, scale, gate_mod, gate_weight, up_weight, down_weight
):
    tok_dev, width = tokens.shape
    experts, depth, units = gate_weight.shape
    capacity = max(2, 3 * tok_dev // experts)
    first_row = (lax.axis_index("dp") * n_owner + lax.axis_index("expert")) * tok_dev
    image = first_row // PIX if shift.shape[0] > 1 else 0
    shift_row = lax.dynamic_slice_in_dim(shift, image, 1, 0)
    scale_row = lax.dynamic_slice_in_dim(scale, image, 1, 0)
    gate_row = lax.dynamic_slice_in_dim(gate_mod, image, 1, 0)
    hot = routes[:, :, None] == jnp.arange(experts, dtype=jnp.int32)[None, None, :]
    named = jnp.sum(hot.astype(jnp.bfloat16), axis=1)
    order = jnp.arange(tok_dev)
    below = (order[:, None] > order[None, :]).astype(jnp.bfloat16)
    rank = jnp.dot(below, named, preferred_element_type=jnp.float32)
    slot = jnp.sum(jnp.where(hot, rank[:, None, :], 0.0), axis=-1).astype(jnp.int32)
    position = routes * capacity + slot
    places = jnp.arange(experts * capacity, dtype=jnp.int32)
    comb = (position.T[:, :, None] == places[None, None, :]).astype(jnp.bfloat16)
    turned = position.T[:, None, :] == places[None, :, None]
    disp = (turned[0] | turned[1]).astype(jnp.bfloat16).reshape(experts, capacity, tok_dev)
    vmem = pl.BlockSpec(memory_space=pltpu.VMEM)
    hbm = pl.BlockSpec(memory_space=pl.ANY)
    grid_rows = n_owner * capacity
    return pl.pallas_call(
        functools.partial(kernel, n_dp, n_owner),
        out_shape=jax.ShapeDtypeStruct((tok_dev, width), jnp.bfloat16),
        in_specs=[vmem] * 8 + [hbm] * 3,
        out_specs=vmem,
        scratch_shapes=[
            pltpu.VMEM((3, n_dp * n_owner, depth, units), jnp.bfloat16),
            pltpu.VMEM((tok_dev, width), jnp.bfloat16),
            pltpu.VMEM((n_owner - 1, capacity, width), jnp.bfloat16),
            pltpu.VMEM((n_owner, capacity, width), jnp.bfloat16),
            pltpu.VMEM((grid_rows, units), jnp.float32),
            pltpu.VMEM((grid_rows, units), jnp.bfloat16),
            pltpu.VMEM((n_owner, n_owner, capacity, n_dp * depth), jnp.bfloat16),
            pltpu.VMEM((n_owner, n_owner, capacity, n_dp * depth), jnp.bfloat16),
            pltpu.VMEM((2, tok_dev, depth), jnp.float32),
            pltpu.SemaphoreType.DMA((3,)),
            pltpu.SemaphoreType.DMA((3, n_owner, 4)),
            pltpu.SemaphoreType.DMA((3, 3)),
            pltpu.SemaphoreType.DMA((1,)),
            pltpu.SemaphoreType.DMA((n_owner,)),
            pltpu.SemaphoreType.DMA((n_owner,)),
            pltpu.SemaphoreType.DMA((n_owner, n_owner)),
        ],
        compiler_params=pltpu.CompilerParams(
            collective_id=0, has_side_effects=True, vmem_limit_bytes=64000 * 1024
        ),
    )(
        tokens, router_weight, routes, shift_row, scale_row, gate_row, disp, comb,
        gate_weight, up_weight, down_weight,
    )


def choose(mesh):
    n_dp, n_owner = mesh.shape["dp"], mesh.shape["expert"]

    def body(*args):
        tokens, weight = args[0], args[6]
        capacity = max(2, 3 * tokens.shape[0] // weight.shape[0])
        fits = n_dp == 4 and weight.shape[0] == n_owner and n_owner % 2 == 0
        fits = fits and capacity % 16 == 0 and weight.shape[1] % 128 == 0 and tokens.shape[0] % 16 == 0
        if fits:
            return shards(n_dp, n_owner, *args)
        return shards_plain(*args)

    return body


def solution(mesh):
    in_specs = (
        P(("dp", "expert"), None),
        P(("dp", "expert"), None),
        P(),
        P(),
        P(),
        P(),
        P(None, ("dp", "expert"), None),
        P(None, ("dp", "expert"), None),
        P(None, ("dp", "expert"), None),
    )
    out_specs = P(("dp", "expert"), None)
    return jax.shard_map(
        choose(mesh), mesh=mesh, in_specs=in_specs, out_specs=out_specs, check_vma=False)
```

```python
import functools

import jax
import jax.numpy as jnp
from jax import lax
from jax.experimental import pallas as pl
from jax.experimental.pallas import tpu as pltpu
from jax.sharding import PartitionSpec as P

PIX = 4096


EPS = 1e-06

LAG, FAR = 2, 1
FAR_TOKENS, GATE_AT = 2, 3


def send_back(output):
    return lax.all_to_all(output, "expert", split_axis=0, concat_axis=0, tiled=True)


def shards_plain(
    tokens, routes, router_weight, shift, scale, gate_mod, gate_weight, up_weight, down_weight
):
    tok_dev = tokens.shape[0]
    width = tokens.shape[1]
    experts = router_weight.shape[1]
    n_owner = lax.axis_size("expert")
    local_count = experts // n_owner
    capacity = max(2, 3 * tok_dev // experts)
    first_row = (lax.axis_index("dp") * n_owner + lax.axis_index("expert")) * tok_dev
    image = first_row // PIX
    shift_row = lax.dynamic_slice_in_dim(shift, image, 1, 0)
    scale_row = lax.dynamic_slice_in_dim(scale, image, 1, 0)
    gate_row = lax.dynamic_slice_in_dim(gate_mod, image, 1, 0)
    values = tokens.astype(jnp.float32)
    meansq = jnp.mean(values * values, axis=-1, keepdims=True)
    normed = (values * lax.rsqrt(meansq + EPS) * (1.0 + scale_row) + shift_row).astype(jnp.bfloat16)
    logits = jnp.dot(normed, router_weight, preferred_element_type=jnp.float32)
    onehot = routes[:, :, None] == jnp.arange(experts, dtype=jnp.int32)[None, None, :]
    chosen = jnp.sum(jnp.where(onehot, logits[:, None, :], 0.0), axis=-1)
    score = jax.nn.sigmoid(chosen)
    flat = routes.reshape(-1)
    hot = (flat[:, None] == jnp.arange(experts, dtype=jnp.int32)[None, :]).astype(jnp.int32)
    rank = jnp.cumsum(hot, axis=0) - hot
    slot = jnp.sum(rank * hot, axis=-1)
    position = flat * capacity + slot
    source = (
        jnp.zeros((experts * capacity,), jnp.int32)
        .at[position]
        .set(jnp.arange(2 * tok_dev, dtype=jnp.int32) // 2)
    )
    filled = jnp.zeros((experts * capacity,), jnp.bool_).at[position].set(True)
    outgoing = jnp.where(filled[:, None], normed[source], jnp.zeros((), jnp.bfloat16)).reshape(
        experts, capacity, width
    )
    quarter_gate, quarter_up, quarter_down = (
        lax.all_to_all(gate_weight, "expert", split_axis=0, concat_axis=1, tiled=True),
        lax.all_to_all(up_weight, "expert", split_axis=0, concat_axis=1, tiled=True),
        lax.all_to_all(down_weight, "expert", split_axis=0, concat_axis=1, tiled=True),
    )
    w_gate, w_up, w_down = (
        lax.all_gather(quarter_gate, "dp", axis=1, tiled=True),
        lax.all_gather(quarter_up, "dp", axis=1, tiled=True),
        lax.all_gather(quarter_down, "dp", axis=1, tiled=True),
    )
    received = lax.all_to_all(outgoing, "expert", split_axis=0, concat_axis=0, tiled=True)
    slots = received.shape[1]
    grid = received.reshape(n_owner, local_count, slots, width)
    gate = jnp.einsum("nxcd,xdf->nxcf", grid, w_gate, preferred_element_type=jnp.float32)
    upper = jnp.einsum("nxcd,xdf->nxcf", grid, w_up, preferred_element_type=jnp.float32)
    hidden = (jax.nn.silu(gate) * upper).astype(jnp.bfloat16)
    output = jnp.einsum(
        "nxcf,xdf->nxcd", hidden, w_down, preferred_element_type=jnp.float32
    ).astype(jnp.bfloat16)
    output = output.reshape(n_owner * local_count, slots, width)
    incoming = send_back(output)
    picked = (
        incoming.reshape(experts * capacity, width)[position]
        .astype(jnp.float32)
        .reshape(tok_dev, 2, width)
    )
    branch = jnp.sum(score[:, :, None] * picked, axis=1)
    return (gate_row * branch).astype(jnp.bfloat16)


MESH = pl.DeviceIdType.MESH


def wait_bytes(ref, sem):
    pltpu.make_async_copy(ref, ref, sem).wait()


def kernel(
    n_dp, n_owner, tok_ref, router_ref, routes_ref, place_ref, shift_ref, scale_ref, gmod_ref,
    gate_ref, up_ref, down_ref, out_ref,
    weights, normed, far_tok, meta, outgoing, rows, gate_acc, hidden, obuf, incoming, comb, dense, land,
    z_send, w_recv, xy_send, f_send, f_recv, t_send, t_recv, h_sem, o_send, o_recv, d_send, d_recv,
):
    dp, me = lax.axis_index("dp"), lax.axis_index("expert")
    x_dp = dp + 1 - 2 * (dp % 2)
    y_dp = (dp + 2) % n_dp
    d_dp = n_dp - 1 - dp
    n_half = n_owner // 2
    half, low = me // n_half, me % n_half
    other = 1 - half
    mirror = other * n_half + low
    tok_dev, width = tok_ref.shape
    capacity = outgoing.shape[2]
    depth, units = gate_ref.shape[1], gate_ref.shape[2]
    args = (gate_ref, up_ref, down_ref)

    barrier = pltpu.get_barrier_semaphore()
    for r in range(1, n_owner):
        pl.semaphore_signal(barrier, inc=1, device_id=(dp, (me + r) % n_owner), device_id_type=MESH)
    pl.semaphore_signal(barrier, inc=1, device_id=(x_dp, me), device_id_type=MESH)
    pl.semaphore_signal(barrier, inc=1, device_id=(y_dp, me), device_id_type=MESH)
    pl.semaphore_wait(barrier, n_owner + 1)

    def remote(src, dst, send_sem, recv_sem, to):
        return pltpu.make_async_remote_copy(
            src_ref=src, dst_ref=dst, send_sem=send_sem, recv_sem=recv_sem, device_id=to, device_id_type=MESH
        )

    def send_column(a):
        at = dp * n_owner + me
        pltpu.make_async_copy(args[a].at[me], weights.at[a, at], w_recv.at[a, 0, 0]).start()
        for r in range(1, n_owner):
            to = ((half + r // n_half) % 2) * n_half + (low + r) % n_half
            remote(args[a].at[to], weights.at[a, at], z_send.at[a], w_recv.at[a, r, 0], (dp, to)).start()

    def send_half():
        for t in range(n_half):
            to = (low + t) % n_half
            for b in range(2):
                src = down_ref.at[b * n_half + to]
                slot = low * 2 + b
                dst, arrive = weights.at[2, dp * n_owner + slot], w_recv.at[2, slot, 0]
                if t == 0:
                    pltpu.make_async_copy(src, dst, arrive).start()
                else:
                    remote(src, dst, z_send.at[2], arrive, (dp, half * n_half + to)).start()

    def piece(a, r, part):
        if a == 2:
            return weights.at[2, part * n_owner + r]
        source = ((half + r // n_half) % 2) * n_half + (low + n_owner - r) % n_half
        return weights.at[a, part * n_owner + source]

    def spread(a, r, part, to, slot, kind):
        held = piece(a, r, part)
        remote(held, held, xy_send.at[a, kind], w_recv.at[a, r, slot], (to, me)).start()

    def arrived(a, r, part, slot):
        wait_bytes(piece(a, r, part), w_recv.at[a, r, slot])

    def relay(a, r):
        arrived(a, r, dp, 0)
        spread(a, r, dp, x_dp, 1, 0)
        spread(a, r, dp, y_dp, 2, 1)

    def corner(a, r):
        arrived(a, r, x_dp, 1)
        if r % 2 == 0:
            spread(a, r, x_dp, y_dp, 3, 2)
        arrived(a, r, y_dp, 2)
        if r % 2 == 1:
            spread(a, r, y_dp, x_dp, 3, 2)

    send_column(0)
    relay(0, 0)

    block = 16

    @pl.loop(0, tok_dev // block)
    def _(i):
        at = pl.ds(pl.multiple_of(i * block, block), block)
        values = tok_ref[at, :].astype(jnp.float32)
        meansq = jnp.mean(values * values, axis=-1, keepdims=True)
        fresh = values * lax.rsqrt(meansq + EPS) * (1.0 + scale_ref[...]) + shift_ref[...]
        normed[at, :] = fresh.astype(jnp.bfloat16)

    remote(normed, far_tok, f_send.at[0], f_recv.at[0], (dp, mirror)).start()
    logits = jnp.dot(normed[...], router_ref[...], preferred_element_type=jnp.float32)
    names = lax.broadcasted_iota(jnp.int32, logits.shape, 1)
    lanes = lax.broadcasted_iota(jnp.int32, meta.shape[1:], 1)
    facts = jnp.zeros(meta.shape[1:], jnp.float32)
    for k in range(2):
        chosen = jnp.sum(jnp.where(routes_ref[:, k : k + 1] == names, logits, 0.0), axis=-1, keepdims=True)
        facts = jnp.where(lanes == k, place_ref[:, k : k + 1].astype(jnp.float32), facts)
        facts = jnp.where(lanes == 2 + k, jax.nn.sigmoid(chosen), facts)
    meta[0] = facts
    remote(meta.at[0], meta.at[1], f_send.at[1], f_recv.at[1], (dp, mirror)).start()

    def dispatch(who):
        source = normed if who == 0 else far_tok
        from_half = half if who == 0 else other
        for t in range(n_half):
            to = (low + t) % n_half
            expert = half * n_half + to
            spots = (expert * capacity + lax.broadcasted_iota(jnp.int32, (tok_dev, capacity), 1)).astype(jnp.float32)
            first = jnp.where(meta[who, :, 0:1] == spots, 1.0, 0.0)
            second = jnp.where(meta[who, :, 1:2] == spots, 1.0, 0.0)
            hot = (first + second).astype(jnp.bfloat16)
            picked = lax.dot_general(
                hot, source[...], (((0,), (0,)), ((), ())), preferred_element_type=jnp.float32
            ).astype(jnp.bfloat16)
            if t == 0:
                rows[low, from_half] = picked
            else:
                outgoing[who, t - 1] = picked
                remote(
                    outgoing.at[who, t - 1], rows.at[low, from_half],
                    t_send.at[who], t_recv.at[who, t], (dp, expert),
                ).start()

    dispatch(0)
    send_column(1)
    send_half()

    def take_far():
        wait_bytes(far_tok, f_recv.at[0])
        wait_bytes(meta.at[1], f_recv.at[1])
        dispatch(1)
        for who in range(2):
            cells = lax.broadcasted_iota(jnp.int32, comb.shape[2:], 1).astype(jnp.float32)
            for k in range(2):
                comb[who, k] = jnp.where(meta[who, :, k : k + 1] == cells, 1.0, 0.0).astype(jnp.bfloat16)

    tile = 256

    def multiply(a):
        for r in range(n_owner):
            arrived(a, r, d_dp, 3)
        if a == 0:
            for who in range(2):
                from_half = half if who == 0 else other
                for t in range(1, n_half):
                    wait_bytes(rows.at[(low + n_half - t) % n_half, from_half], t_recv.at[who, t])

        @pl.loop(0, units // tile)
        def _(i):
            at = pl.ds(pl.multiple_of(i * tile, tile), tile)
            part = weights[a, :, :, at].reshape(width, tile)
            grid = rows[...].reshape(n_owner * capacity, width)
            result = jnp.dot(grid, part, preferred_element_type=jnp.float32)
            if a == 0:
                gate_acc[:, at] = result
            else:
                hidden[half, :, at] = (jax.nn.silu(gate_acc[:, at]) * result).astype(jnp.bfloat16)

        if a == 1:
            remote(hidden.at[half], hidden.at[half], h_sem.at[0], h_sem.at[1], (dp, mirror)).start()

    def finish(s):
        if s == 0:
            wait_bytes(hidden.at[other], h_sem.at[1])
        for b in range(2):
            r = s * 2 + b
            arrived(2, r, d_dp, 3)
            for q in range(n_dp):
                result = lax.dot_general(
                    hidden[b], weights[2, q * n_owner + r], (((1,), (1,)), ((), ())),
                    preferred_element_type=jnp.float32,
                ).astype(jnp.bfloat16)
                obuf[s, b, :, :, :, q * depth : (q + 1) * depth] = result.reshape(n_half, 2, capacity, depth)
            incoming[s, b * n_half + low] = obuf[s, b, low]
            for t in range(1, n_half):
                to = (low + t) % n_half
                remote(
                    obuf.at[s, b, to], incoming.at[s, b * n_half + low],
                    o_send.at[s], o_recv.at[s, b, t], (dp, half * n_half + to),
                ).start()

    def columns(q, part, s):
        return pl.ds(pl.multiple_of(((q * 2 + part) * n_half + s) * depth, depth), depth)

    def combine(s):
        for b in range(2):
            for t in range(1, n_half):
                sender = b * n_half + (low + n_half - t) % n_half
                wait_bytes(incoming.at[s, sender], o_recv.at[s, b, t])
        for who in (1, 0):
            block_in = incoming[s, :, half if who == 0 else other].reshape(n_owner * capacity, n_dp * depth)
            first = jnp.dot(comb[who, 0], block_in, preferred_element_type=jnp.float32)
            second = jnp.dot(comb[who, 1], block_in, preferred_element_type=jnp.float32)
            branch = meta[who, :, 2:3] * first + meta[who, :, 3:4] * second
            for q in range(n_dp):
                at = columns(q, half, s)
                value = (gmod_ref[:, at] * branch[:, q * depth : (q + 1) * depth]).astype(jnp.bfloat16)
                if who == 0:
                    out_ref[:, at] = value
                else:
                    dense[s, :, q * depth : (q + 1) * depth] = value
            if who == 1:
                remote(dense.at[s], land.at[s], d_send.at[0], d_recv.at[s], (dp, mirror)).start()

    lag, far = LAG, FAR
    pieces = 3 * n_owner
    for k in range(1, pieces + lag + far):
        if k == n_owner + FAR_TOKENS:
            take_far()
        if k < pieces:
            relay(*divmod(k, n_owner))
        if lag <= k < pieces + lag:
            corner(*divmod(k - lag, n_owner))
        if k >= lag + far:
            a, r = divmod(k - lag - far, n_owner)
            if (a, r) == (1, GATE_AT):
                multiply(0)
            if (a, r) == (1, n_owner - 1):
                multiply(1)
            if a == 2 and r % 2 == 1:
                finish(r // 2)
                if r > 1:
                    combine(r // 2 - 1)
    combine(n_half - 1)
    for s in range(n_half):
        wait_bytes(land.at[s], d_recv.at[s])
        for q in range(n_dp):
            out_ref[:, columns(q, other, s)] = land[s, :, q * depth : (q + 1) * depth]

    for a in range(3):
        count = n_owner - 1 if a < 2 else n_owner - 2
        wait_bytes(args[a].at[pl.ds(0, count)], z_send.at[a])
        for kind in range(3):
            wait_bytes(weights.at[a, pl.ds(0, n_owner)], xy_send.at[a, kind])
    wait_bytes(normed, f_send.at[0])
    wait_bytes(meta.at[0], f_send.at[1])
    for who in range(2):
        wait_bytes(outgoing.at[who], t_send.at[who])
    wait_bytes(hidden.at[half], h_sem.at[0])
    for s in range(n_half):
        wait_bytes(incoming.at[s, pl.ds(0, n_owner - 2)], o_send.at[s])
    wait_bytes(dense, d_send.at[0])


def shards(
    n_dp, n_owner, tokens, routes, router_weight, shift, scale, gate_mod, gate_weight, up_weight, down_weight
):
    tok_dev, width = tokens.shape
    experts, depth, units = gate_weight.shape
    capacity = max(2, 3 * tok_dev // experts)
    first_row = (lax.axis_index("dp") * n_owner + lax.axis_index("expert")) * tok_dev
    image = first_row // PIX if shift.shape[0] > 1 else 0
    shift_row = lax.dynamic_slice_in_dim(shift, image, 1, 0)
    scale_row = lax.dynamic_slice_in_dim(scale, image, 1, 0)
    gate_row = lax.dynamic_slice_in_dim(gate_mod, image, 1, 0)
    hot = routes[:, :, None] == jnp.arange(experts, dtype=jnp.int32)[None, None, :]
    named = jnp.sum(hot.astype(jnp.bfloat16), axis=1)
    order = jnp.arange(tok_dev)
    below = (order[:, None] > order[None, :]).astype(jnp.bfloat16)
    rank = jnp.dot(below, named, preferred_element_type=jnp.float32)
    slot = jnp.sum(jnp.where(hot, rank[:, None, :], 0.0), axis=-1).astype(jnp.int32)
    place = routes * capacity + slot
    vmem = pl.BlockSpec(memory_space=pltpu.VMEM)
    hbm = pl.BlockSpec(memory_space=pl.ANY)
    grid_rows = n_owner * capacity
    n_half = n_owner // 2
    return pl.pallas_call(
        functools.partial(kernel, n_dp, n_owner),
        out_shape=jax.ShapeDtypeStruct((tok_dev, width), jnp.bfloat16),
        in_specs=[vmem] * 7 + [hbm] * 3,
        out_specs=vmem,
        scratch_shapes=[
            pltpu.VMEM((3, n_dp * n_owner, depth, units), jnp.bfloat16),
            pltpu.VMEM((tok_dev, width), jnp.bfloat16),
            pltpu.VMEM((tok_dev, width), jnp.bfloat16),
            pltpu.VMEM((2, tok_dev, 128), jnp.float32),
            pltpu.VMEM((2, n_half - 1, capacity, width), jnp.bfloat16),
            pltpu.VMEM((n_half, 2, capacity, width), jnp.bfloat16),
            pltpu.VMEM((grid_rows, units), jnp.float32),
            pltpu.VMEM((2, grid_rows, units), jnp.bfloat16),
            pltpu.VMEM((n_half, 2, n_half, 2, capacity, n_dp * depth), jnp.bfloat16),
            pltpu.VMEM((n_half, n_owner, 2, capacity, n_dp * depth), jnp.bfloat16),
            pltpu.VMEM((2, 2, tok_dev, grid_rows), jnp.bfloat16),
            pltpu.VMEM((n_half, tok_dev, n_dp * depth), jnp.bfloat16),
            pltpu.VMEM((n_half, tok_dev, n_dp * depth), jnp.bfloat16),
            pltpu.SemaphoreType.DMA((3,)),
            pltpu.SemaphoreType.DMA((3, n_owner, 4)),
            pltpu.SemaphoreType.DMA((3, 3)),
            pltpu.SemaphoreType.DMA((2,)),
            pltpu.SemaphoreType.DMA((2,)),
            pltpu.SemaphoreType.DMA((2,)),
            pltpu.SemaphoreType.DMA((2, n_half)),
            pltpu.SemaphoreType.DMA((2,)),
            pltpu.SemaphoreType.DMA((n_half,)),
            pltpu.SemaphoreType.DMA((n_half, 2, n_half)),
            pltpu.SemaphoreType.DMA((1,)),
            pltpu.SemaphoreType.DMA((n_half,)),
        ],
        compiler_params=pltpu.CompilerParams(
            collective_id=0, has_side_effects=True, vmem_limit_bytes=64000 * 1024
        ),
    )(
        tokens, router_weight, routes, place, shift_row, scale_row, gate_row,
        gate_weight, up_weight, down_weight,
    )


def choose(mesh):
    n_dp, n_owner = mesh.shape["dp"], mesh.shape["expert"]

    def body(*args):
        tokens, weight = args[0], args[6]
        capacity = max(2, 3 * tokens.shape[0] // weight.shape[0])
        fits = n_dp == 4 and weight.shape[0] == n_owner and n_owner % 2 == 0
        fits = fits and capacity % 16 == 0 and weight.shape[1] % 128 == 0 and tokens.shape[0] % 16 == 0
        fits = fits and PIX % (n_owner * tokens.shape[0]) == 0
        if fits:
            return shards(n_dp, n_owner, *args)
        return shards_plain(*args)

    return body


def solution(mesh):
    in_specs = (
        P(("dp", "expert"), None),
        P(("dp", "expert"), None),
        P(),
        P(),
        P(),
        P(),
        P(None, ("dp", "expert"), None),
        P(None, ("dp", "expert"), None),
        P(None, ("dp", "expert"), None),
    )
    out_specs = P(("dp", "expert"), None)
    return jax.shard_map(
        choose(mesh), mesh=mesh, in_specs=in_specs, out_specs=out_specs, check_vma=False)
```

```python
import functools

import jax
import jax.numpy as jnp
from jax import lax
from jax.experimental import pallas as pl
from jax.experimental.pallas import tpu as pltpu
from jax.sharding import PartitionSpec as P

PIX = 4096


EPS = 1e-06

LAG, FAR = 1, 1
ISSUE = (1, 1)
FAR_TOKENS = 12
MULTIPLY = (13, 15)


def send_back(output):
    return lax.all_to_all(output, "expert", split_axis=0, concat_axis=0, tiled=True)


def shards_plain(
    tokens, routes, router_weight, shift, scale, gate_mod, gate_weight, up_weight, down_weight
):
    tok_dev = tokens.shape[0]
    width = tokens.shape[1]
    experts = router_weight.shape[1]
    n_owner = lax.axis_size("expert")
    local_count = experts // n_owner
    capacity = max(2, 3 * tok_dev // experts)
    first_row = (lax.axis_index("dp") * n_owner + lax.axis_index("expert")) * tok_dev
    image = first_row // PIX
    shift_row = lax.dynamic_slice_in_dim(shift, image, 1, 0)
    scale_row = lax.dynamic_slice_in_dim(scale, image, 1, 0)
    gate_row = lax.dynamic_slice_in_dim(gate_mod, image, 1, 0)
    values = tokens.astype(jnp.float32)
    meansq = jnp.mean(values * values, axis=-1, keepdims=True)
    normed = (values * lax.rsqrt(meansq + EPS) * (1.0 + scale_row) + shift_row).astype(jnp.bfloat16)
    logits = jnp.dot(normed, router_weight, preferred_element_type=jnp.float32)
    onehot = routes[:, :, None] == jnp.arange(experts, dtype=jnp.int32)[None, None, :]
    chosen = jnp.sum(jnp.where(onehot, logits[:, None, :], 0.0), axis=-1)
    score = jax.nn.sigmoid(chosen)
    flat = routes.reshape(-1)
    hot = (flat[:, None] == jnp.arange(experts, dtype=jnp.int32)[None, :]).astype(jnp.int32)
    rank = jnp.cumsum(hot, axis=0) - hot
    slot = jnp.sum(rank * hot, axis=-1)
    position = flat * capacity + slot
    source = (
        jnp.zeros((experts * capacity,), jnp.int32)
        .at[position]
        .set(jnp.arange(2 * tok_dev, dtype=jnp.int32) // 2)
    )
    filled = jnp.zeros((experts * capacity,), jnp.bool_).at[position].set(True)
    outgoing = jnp.where(filled[:, None], normed[source], jnp.zeros((), jnp.bfloat16)).reshape(
        experts, capacity, width
    )
    quarter_gate, quarter_up, quarter_down = (
        lax.all_to_all(gate_weight, "expert", split_axis=0, concat_axis=1, tiled=True),
        lax.all_to_all(up_weight, "expert", split_axis=0, concat_axis=1, tiled=True),
        lax.all_to_all(down_weight, "expert", split_axis=0, concat_axis=1, tiled=True),
    )
    w_gate, w_up, w_down = (
        lax.all_gather(quarter_gate, "dp", axis=1, tiled=True),
        lax.all_gather(quarter_up, "dp", axis=1, tiled=True),
        lax.all_gather(quarter_down, "dp", axis=1, tiled=True),
    )
    received = lax.all_to_all(outgoing, "expert", split_axis=0, concat_axis=0, tiled=True)
    slots = received.shape[1]
    grid = received.reshape(n_owner, local_count, slots, width)
    gate = jnp.einsum("nxcd,xdf->nxcf", grid, w_gate, preferred_element_type=jnp.float32)
    upper = jnp.einsum("nxcd,xdf->nxcf", grid, w_up, preferred_element_type=jnp.float32)
    hidden = (jax.nn.silu(gate) * upper).astype(jnp.bfloat16)
    output = jnp.einsum(
        "nxcf,xdf->nxcd", hidden, w_down, preferred_element_type=jnp.float32
    ).astype(jnp.bfloat16)
    output = output.reshape(n_owner * local_count, slots, width)
    incoming = send_back(output)
    picked = (
        incoming.reshape(experts * capacity, width)[position]
        .astype(jnp.float32)
        .reshape(tok_dev, 2, width)
    )
    branch = jnp.sum(score[:, :, None] * picked, axis=1)
    return (gate_row * branch).astype(jnp.bfloat16)


MESH = pl.DeviceIdType.MESH


def wait_bytes(ref, sem):
    pltpu.make_async_copy(ref, ref, sem).wait()


def kernel(
    n_dp, n_owner, tok_ref, router_ref, routes_ref, place_ref, shift_ref, scale_ref, gmod_ref,
    gate_ref, up_ref, down_ref, out_ref,
    weights, downs, normed, far_tok, meta, outgoing, rows, gate_acc, hidden, obuf, incoming, comb, dense, land,
    z_send, w_recv, xy_send, f_send, f_recv, t_send, t_recv, h_send, h_recv, o_send, o_recv, d_send, d_recv,
):
    dp, me = lax.axis_index("dp"), lax.axis_index("expert")
    x_dp = dp + 1 - 2 * (dp % 2)
    y_dp = (dp + 2) % n_dp
    d_dp = n_dp - 1 - dp
    n_half = n_owner // 2
    half, low = me // n_half, me % n_half
    other = 1 - half
    mirror = other * n_half + low
    tok_dev, width = tok_ref.shape
    capacity = outgoing.shape[2]
    depth, units = gate_ref.shape[1], gate_ref.shape[2]
    span = units
    last = 2

    def argument(a, expert):
        return (gate_ref, up_ref)[a].at[expert]

    barrier = pltpu.get_barrier_semaphore()
    for r in range(1, n_owner):
        pl.semaphore_signal(barrier, inc=1, device_id=(dp, (me + r) % n_owner), device_id_type=MESH)
    pl.semaphore_signal(barrier, inc=1, device_id=(x_dp, me), device_id_type=MESH)
    pl.semaphore_signal(barrier, inc=1, device_id=(y_dp, me), device_id_type=MESH)
    pl.semaphore_wait(barrier, n_owner + 1)

    def remote(src, dst, send_sem, recv_sem, to):
        return pltpu.make_async_remote_copy(
            src_ref=src, dst_ref=dst, send_sem=send_sem, recv_sem=recv_sem, device_id=to, device_id_type=MESH
        )

    def send_column(a):
        at = dp * n_owner + me
        pltpu.make_async_copy(argument(a, me), weights.at[a, at], w_recv.at[a, 0, 0]).start()
        for r in range(1, n_owner):
            to = ((half + r // n_half) % 2) * n_half + (low + r) % n_half
            remote(argument(a, to), weights.at[a, at], z_send.at[a], w_recv.at[a, r, 0], (dp, to)).start()

    def send_half():
        for b in range(2):
            for t in range(n_half):
                to = (low + t) % n_half
                src = down_ref.at[((half + b) % 2) * n_half + to]
                slot = b * n_half + low
                dst, arrive = downs.at[dp * n_owner + slot], w_recv.at[last, slot, 0]
                if t == 0:
                    pltpu.make_async_copy(src, dst, arrive).start()
                else:
                    remote(src, dst, z_send.at[last], arrive, (dp, half * n_half + to)).start()

    def piece(a, r, part):
        if a == last:
            return downs.at[part * n_owner + r]
        source = ((half + r // n_half) % 2) * n_half + (low + n_owner - r) % n_half
        return weights.at[a, part * n_owner + source]

    def spread(a, r, part, to, slot, kind):
        held = piece(a, r, part)
        remote(held, held, xy_send.at[a, kind], w_recv.at[a, r, slot], (to, me)).start()

    def arrived(a, r, part, slot):
        wait_bytes(piece(a, r, part), w_recv.at[a, r, slot])

    def relay(a, r):
        arrived(a, r, dp, 0)
        spread(a, r, dp, x_dp, 1, 0)
        spread(a, r, dp, y_dp, 2, 1)

    def corner(a, r):
        arrived(a, r, x_dp, 1)
        if r % 2 == 0:
            spread(a, r, x_dp, y_dp, 3, 2)
        arrived(a, r, y_dp, 2)
        if r % 2 == 1:
            spread(a, r, y_dp, x_dp, 3, 2)

    send_column(0)
    relay(0, 0)

    block = 16

    @pl.loop(0, tok_dev // block)
    def _(i):
        at = pl.ds(pl.multiple_of(i * block, block), block)
        values = tok_ref[at, :].astype(jnp.float32)
        meansq = jnp.mean(values * values, axis=-1, keepdims=True)
        fresh = values * lax.rsqrt(meansq + EPS) * (1.0 + scale_ref[...]) + shift_ref[...]
        normed[at, :] = fresh.astype(jnp.bfloat16)

    remote(normed, far_tok, f_send.at[0], f_recv.at[0], (dp, mirror)).start()
    logits = jnp.dot(normed[...], router_ref[...], preferred_element_type=jnp.float32)
    names = lax.broadcasted_iota(jnp.int32, logits.shape, 1)
    lanes = lax.broadcasted_iota(jnp.int32, meta.shape[1:], 1)
    facts = jnp.zeros(meta.shape[1:], jnp.float32)
    for k in range(2):
        chosen = jnp.sum(jnp.where(routes_ref[:, k : k + 1] == names, logits, 0.0), axis=-1, keepdims=True)
        facts = jnp.where(lanes == k, place_ref[:, k : k + 1].astype(jnp.float32), facts)
        facts = jnp.where(lanes == 2 + k, jax.nn.sigmoid(chosen), facts)
    meta[0] = facts
    remote(meta.at[0], meta.at[1], f_send.at[1], f_recv.at[1], (dp, mirror)).start()

    def dispatch(who):
        source = normed if who == 0 else far_tok
        from_half = half if who == 0 else other
        for t in range(n_half):
            to = (low + t) % n_half
            expert = half * n_half + to
            spots = (expert * capacity + lax.broadcasted_iota(jnp.int32, (tok_dev, capacity), 1)).astype(jnp.float32)
            first = jnp.where(meta[who, :, 0:1] == spots, 1.0, 0.0)
            second = jnp.where(meta[who, :, 1:2] == spots, 1.0, 0.0)
            hot = (first + second).astype(jnp.bfloat16)
            picked = lax.dot_general(
                hot, source[...], (((0,), (0,)), ((), ())), preferred_element_type=jnp.float32
            ).astype(jnp.bfloat16)
            if t == 0:
                rows[low, from_half] = picked
            else:
                outgoing[who, t - 1] = picked
                remote(
                    outgoing.at[who, t - 1], rows.at[low, from_half],
                    t_send.at[who], t_recv.at[who, t], (dp, expert),
                ).start()

    dispatch(0)

    def take_far():
        wait_bytes(far_tok, f_recv.at[0])
        wait_bytes(meta.at[1], f_recv.at[1])
        dispatch(1)
        for who in range(2):
            cells = lax.broadcasted_iota(jnp.int32, comb.shape[2:], 1).astype(jnp.float32)
            for k in range(2):
                comb[who, k] = jnp.where(meta[who, :, k : k + 1] == cells, 1.0, 0.0).astype(jnp.bfloat16)

    tile = 256

    def multiply(a):
        for r in range(n_owner):
            arrived(a, r, d_dp, 3)
        if a == 0:
            for who in range(2):
                from_half = half if who == 0 else other
                for t in range(1, n_half):
                    wait_bytes(rows.at[(low + n_half - t) % n_half, from_half], t_recv.at[who, t])

        @pl.loop(0, span // tile)
        def _(i):
            at = pl.ds(pl.multiple_of(i * tile, tile), tile)
            part = weights[a, :, :, at].reshape(width, tile)
            grid = rows[...].reshape(n_owner * capacity, width)
            result = jnp.dot(grid, part, preferred_element_type=jnp.float32)
            if a % 2 == 0:
                gate_acc[:, at] = result
            else:
                hidden[0, a // 2, :, at] = (jax.nn.silu(gate_acc[:, at]) * result).astype(jnp.bfloat16)

        if a % 2 == 1:
            remote(hidden.at[0, a // 2], hidden.at[1, a // 2], h_send.at[a // 2], h_recv.at[a // 2], (dp, mirror)).start()

    def finish(r):
        b, s = divmod(r, n_half)
        if r == n_half:
            for side in range(1):
                wait_bytes(hidden.at[1, side], h_recv.at[side])
        arrived(last, r, d_dp, 3)
        expert = ((half + b) % 2) * n_half + low
        for q in range(n_dp):
            total = jnp.zeros((n_owner * capacity, depth), jnp.float32)
            for side in range(1):
                total += lax.dot_general(
                    hidden[b, side], downs[q * n_owner + r, :, side * span : (side + 1) * span],
                    (((1,), (1,)), ((), ())), preferred_element_type=jnp.float32,
                )
            result = total.astype(jnp.bfloat16).reshape(n_half, 2, capacity, depth)
            obuf[r, :, :, :, q * depth : (q + 1) * depth] = result
        incoming[s, expert] = obuf[r, low]
        for t in range(1, n_half):
            to = (low + t) % n_half
            remote(
                obuf.at[r, to], incoming.at[s, expert],
                o_send.at[r], o_recv.at[s, b, t], (dp, half * n_half + to),
            ).start()

    def columns(q, part, s):
        return pl.ds(pl.multiple_of(((q * 2 + part) * n_half + s) * depth, depth), depth)

    def combine(s):
        for b in range(2):
            for t in range(1, n_half):
                sender = ((half + b) % 2) * n_half + (low + n_half - t) % n_half
                wait_bytes(incoming.at[s, sender], o_recv.at[s, b, t])
        for who in (1, 0):
            block_in = incoming[s, :, half if who == 0 else other].reshape(n_owner * capacity, n_dp * depth)
            first = jnp.dot(comb[who, 0], block_in, preferred_element_type=jnp.float32)
            second = jnp.dot(comb[who, 1], block_in, preferred_element_type=jnp.float32)
            branch = meta[who, :, 2:3] * first + meta[who, :, 3:4] * second
            for q in range(n_dp):
                at = columns(q, half, s)
                value = (gmod_ref[:, at] * branch[:, q * depth : (q + 1) * depth]).astype(jnp.bfloat16)
                if who == 0:
                    out_ref[:, at] = value
                else:
                    dense[s, :, q * depth : (q + 1) * depth] = value
            if who == 1:
                remote(dense.at[s], land.at[s], d_send.at[0], d_recv.at[s], (dp, mirror)).start()

    lag, far = LAG, FAR
    steps = [(a, r) for a in range(last + 1) for r in range(n_owner)]
    for k in range(1, len(steps) + lag + far):
        for a in range(1, last + 1):
            if k == ISSUE[a - 1]:
                send_half() if a == last else send_column(a)
        if k == FAR_TOKENS:
            take_far()
        if k < len(steps):
            relay(*steps[k])
        if lag <= k < len(steps) + lag:
            corner(*steps[k - lag])
        if k >= lag + far:
            a, r = steps[k - lag - far]
            for half_step in range(last):
                if (a * n_owner + r) == MULTIPLY[half_step]:
                    multiply(half_step)
            if a == last:
                finish(r)
                if r > n_half:
                    combine(r - n_half - 1)
    combine(n_half - 1)
    for s in range(n_half):
        wait_bytes(land.at[s], d_recv.at[s])
        for q in range(n_dp):
            out_ref[:, columns(q, other, s)] = land[s, :, q * depth : (q + 1) * depth]

    for a in range(last + 1):
        held = downs if a == last else weights.at[a]
        wait_bytes(held.at[pl.ds(0, n_owner - 2 if a == last else n_owner - 1)], z_send.at[a])
        for kind in range(3):
            wait_bytes(held.at[pl.ds(0, n_owner)], xy_send.at[a, kind])
    wait_bytes(normed, f_send.at[0])
    wait_bytes(meta.at[0], f_send.at[1])
    for who in range(2):
        wait_bytes(outgoing.at[who], t_send.at[who])
    for side in range(1):
        wait_bytes(hidden.at[0, side], h_send.at[side])
    for r in range(n_owner):
        wait_bytes(obuf.at[r, pl.ds(0, n_half - 1)], o_send.at[r])
    wait_bytes(dense, d_send.at[0])


def shards(
    n_dp, n_owner, tokens, routes, router_weight, shift, scale, gate_mod, gate_weight, up_weight, down_weight
):
    tok_dev, width = tokens.shape
    experts, depth, units = gate_weight.shape
    capacity = max(2, 3 * tok_dev // experts)
    first_row = (lax.axis_index("dp") * n_owner + lax.axis_index("expert")) * tok_dev
    image = first_row // PIX if shift.shape[0] > 1 else 0
    shift_row = lax.dynamic_slice_in_dim(shift, image, 1, 0)
    scale_row = lax.dynamic_slice_in_dim(scale, image, 1, 0)
    gate_row = lax.dynamic_slice_in_dim(gate_mod, image, 1, 0)
    hot = routes[:, :, None] == jnp.arange(experts, dtype=jnp.int32)[None, None, :]
    named = jnp.sum(hot.astype(jnp.bfloat16), axis=1)
    order = jnp.arange(tok_dev)
    below = (order[:, None] > order[None, :]).astype(jnp.bfloat16)
    rank = jnp.dot(below, named, preferred_element_type=jnp.float32)
    slot = jnp.sum(jnp.where(hot, rank[:, None, :], 0.0), axis=-1).astype(jnp.int32)
    place = routes * capacity + slot
    vmem = pl.BlockSpec(memory_space=pltpu.VMEM)
    hbm = pl.BlockSpec(memory_space=pl.ANY)
    grid_rows = n_owner * capacity
    n_half = n_owner // 2
    return pl.pallas_call(
        functools.partial(kernel, n_dp, n_owner),
        out_shape=jax.ShapeDtypeStruct((tok_dev, width), jnp.bfloat16),
        in_specs=[vmem] * 7 + [hbm] * 3,
        out_specs=vmem,
        scratch_shapes=[
            pltpu.VMEM((2, n_dp * n_owner, depth, units), jnp.bfloat16),
            pltpu.VMEM((n_dp * n_owner, depth, units), jnp.bfloat16),
            pltpu.VMEM((tok_dev, width), jnp.bfloat16),
            pltpu.VMEM((tok_dev, width), jnp.bfloat16),
            pltpu.VMEM((2, tok_dev, 128), jnp.float32),
            pltpu.VMEM((2, n_half - 1, capacity, width), jnp.bfloat16),
            pltpu.VMEM((n_half, 2, capacity, width), jnp.bfloat16),
            pltpu.VMEM((grid_rows, units), jnp.float32),
            pltpu.VMEM((2, 1, grid_rows, units), jnp.bfloat16),
            pltpu.VMEM((n_owner, n_half, 2, capacity, n_dp * depth), jnp.bfloat16),
            pltpu.VMEM((n_half, n_owner, 2, capacity, n_dp * depth), jnp.bfloat16),
            pltpu.VMEM((2, 2, tok_dev, grid_rows), jnp.bfloat16),
            pltpu.VMEM((n_half, tok_dev, n_dp * depth), jnp.bfloat16),
            pltpu.VMEM((n_half, tok_dev, n_dp * depth), jnp.bfloat16),
            pltpu.SemaphoreType.DMA((3,)),
            pltpu.SemaphoreType.DMA((3, n_owner, 4)),
            pltpu.SemaphoreType.DMA((3, 3)),
            pltpu.SemaphoreType.DMA((2,)),
            pltpu.SemaphoreType.DMA((2,)),
            pltpu.SemaphoreType.DMA((2,)),
            pltpu.SemaphoreType.DMA((2, n_half)),
            pltpu.SemaphoreType.DMA((1,)),
            pltpu.SemaphoreType.DMA((1,)),
            pltpu.SemaphoreType.DMA((n_owner,)),
            pltpu.SemaphoreType.DMA((n_half, 2, n_half)),
            pltpu.SemaphoreType.DMA((1,)),
            pltpu.SemaphoreType.DMA((n_half,)),
        ],
        compiler_params=pltpu.CompilerParams(
            collective_id=0, has_side_effects=True, vmem_limit_bytes=64000 * 1024
        ),
    )(
        tokens, router_weight, routes, place, shift_row, scale_row, gate_row,
        gate_weight, up_weight, down_weight,
    )


def choose(mesh):
    n_dp, n_owner = mesh.shape["dp"], mesh.shape["expert"]

    def body(*args):
        tokens, weight = args[0], args[6]
        capacity = max(2, 3 * tokens.shape[0] // weight.shape[0])
        fits = n_dp == 4 and weight.shape[0] == n_owner and n_owner % 2 == 0
        fits = fits and capacity % 16 == 0 and weight.shape[1] % 128 == 0 and tokens.shape[0] % 16 == 0
        fits = fits and weight.shape[2] % 512 == 0 and PIX % (n_owner * tokens.shape[0]) == 0
        if fits:
            return shards(n_dp, n_owner, *args)
        return shards_plain(*args)

    return body


def solution(mesh):
    in_specs = (
        P(("dp", "expert"), None),
        P(("dp", "expert"), None),
        P(),
        P(),
        P(),
        P(),
        P(None, ("dp", "expert"), None),
        P(None, ("dp", "expert"), None),
        P(None, ("dp", "expert"), None),
    )
    out_specs = P(("dp", "expert"), None)
    return jax.shard_map(
        choose(mesh), mesh=mesh, in_specs=in_specs, out_specs=out_specs, check_vma=False)
```
